16 devices in a mesh: frag: 2 (over y, z), dev: 8 (over x, core).
Axes of the slice: x: 4, y: 2, z: 1, core: 2. Of those that a mesh axis runs over, the one named last changes fastest.
The devices are a block of a 4x4x8 slice.
Arguments:
- ao_ints: bfloat16 [272, 136, 136, 136], P(('frag', 'dev')), parts along dimension 0
- occ_coef: bfloat16 [272, 54], P('frag'), parts along dimension 0
- virt_coef: bfloat16 [272, 56], P('frag'), parts along dimension 0
Outputs:
- output: float32 [108, 56, 3024], P('frag', None, 'dev'), parts along dimension 0
There are 2 independent parts. The reference program is written for one: setup_inputs(seed, part) draws one part's arguments, and reference() takes and returns one part's arrays. A program takes and returns all parts, laid end to end along the dimension named above; each array names one.
All inputs are finite; a program needn't handle non-finite values.
Results may differ from the reference program's by a relative error of at most 0.001.
Values are sent between devices in bfloat16 or wider.
A program may use at most 768 MiB of HBM per device.

```python
import jax
import jax.numpy as jnp
from jax import lax

AO_DIM = 136
OCC_DIM = 54
VIRT_DIM = 56


def setup_inputs(seed: int = 0, part: int = 0) -> dict:
    base_key = jax.random.fold_in(jax.random.key(seed), part)
    key_ints, key_occ, key_virt = jax.random.split(base_key, 3)
    row_keys = jax.random.split(key_ints, AO_DIM)

    def draw_row(row_key):
        return jax.random.normal(row_key, (AO_DIM, AO_DIM, AO_DIM), jnp.float32).astype(jnp.bfloat16)

    ao_ints = lax.map(draw_row, row_keys)
    coef_scale = AO_DIM ** -0.5
    occ_coef = jax.random.normal(key_occ, (AO_DIM, OCC_DIM), jnp.float32) * coef_scale
    virt_coef = jax.random.normal(key_virt, (AO_DIM, VIRT_DIM), jnp.float32) * coef_scale
    return {"ao_ints": ao_ints, "occ_coef": occ_coef.astype(jnp.bfloat16), "virt_coef": virt_coef.astype(jnp.bfloat16)}


def reference(ao_ints, occ_coef, virt_coef):
    occ_wide = occ_coef.astype(jnp.float32)
    virt_wide = virt_coef.astype(jnp.float32)

    def first_half(ao_row):
        quarter = jnp.einsum("qrs,rj->qsj", ao_row.astype(jnp.float32), occ_wide).astype(jnp.bfloat16)
        half_row = jnp.einsum("qsj,sb->qjb", quarter.astype(jnp.float32), virt_wide).astype(jnp.bfloat16)
        return half_row.reshape(AO_DIM, OCC_DIM * VIRT_DIM)

    half_ints = lax.map(first_half, ao_ints)
    three_quarter = jnp.einsum("qa,pqc->apc", virt_wide, half_ints.astype(jnp.float32)).astype(jnp.bfloat16)
    return jnp.einsum("pi,apc->iac", occ_wide, three_quarter.astype(jnp.float32))
```

```python
import functools

import jax
import jax.numpy as jnp
from jax import lax
from jax.experimental import pallas as pl
from jax.experimental.pallas import tpu as pltpu
from jax.sharding import PartitionSpec as P

LANES = 128
SUBL = 8
Q_CHUNK = 34
SLOTS = 2
SKEW = 4
HS = 137


def _up(x, m):
    return -(-x // m) * m


def _half_kernel(ndev, cblk, ao, cot, cvt, g_out, abuf, co_s, cv_s, hbuf, gbuf, asem, gsem):
    rows, n = ao.shape[0], ao.shape[1]
    occ, virt = cot.shape[0], cvt.shape[0]
    occ_p = _up(occ, SUBL)
    nch = n // Q_CHUNK
    steps = rows * nch

    co_s[...] = jnp.zeros(co_s.shape, co_s.dtype)
    co_s[0:occ, :] = cot[...]
    cv_s[...] = jnp.zeros(cv_s.shape, cv_s.dtype)
    cv_s[:, 0:virt] = cvt[...].astype(jnp.float32).T.astype(jnp.bfloat16)

    def fetch(step):
        slot = lax.rem(step, SLOTS)
        p, ch = step // nch, lax.rem(step, nch)
        return pltpu.make_async_copy(
            ao.at[p, pl.ds(ch * Q_CHUNK, Q_CHUNK)], abuf.at[slot], asem.at[slot]
        )

    for s in range(SLOTS):
        fetch(s).start()

    def put(p, slot):
        return pltpu.make_async_copy(gbuf.at[slot], g_out.at[:, p], gsem.at[slot])

    def row(p, carry):
        def chunk(ch, c):
            step = p * nch + ch
            slot = lax.rem(step, SLOTS)
            fetch(step).wait()
            def first(k):
                t = [
                    jnp.dot(co_s[...], abuf[slot, k + i], preferred_element_type=jnp.float32)
                    for i in range(2)
                ]
                return jnp.concatenate(t, axis=0).astype(jnp.bfloat16)

            def second(k, t):
                h = jnp.dot(t, cv_s[...], preferred_element_type=jnp.float32)
                for i in range(2):
                    q = ch * Q_CHUNK + k + i
                    hbuf[pl.ds(q, occ_p, stride=HS), :] = h[i * occ_p : (i + 1) * occ_p]

            pend = []
            for k in range(0, Q_CHUNK, 2):
                pend.append((k, first(k)))
                if len(pend) > SKEW:
                    second(*pend.pop(0))
            for item in pend:
                second(*item)

            @pl.when(step + SLOTS < steps)
            def _():
                fetch(step + SLOTS).start()

            return c

        lax.fori_loop(0, nch, chunk, 0)

        gslot = lax.rem(p, 2)

        @pl.when(p >= 2)
        def _():
            put(p - 2, gslot).wait()

        for j in range(0, occ, 2):
            hh = [hbuf[(j + i) * HS : (j + i) * HS + n, :] for i in range(2)]
            hh = jnp.concatenate(hh, axis=1).astype(jnp.bfloat16)
            g = jnp.dot(cvt[...], hh, preferred_element_type=jnp.float32).astype(jnp.bfloat16)
            for i in range(2):
                c0, base, left = (j + i) * virt, i * LANES, virt
                while left:
                    d, l = c0 // cblk, c0 % cblk
                    w = min(left, cblk - l)
                    gbuf[gslot, d, :, l : l + w] = g[:, base : base + w]
                    c0, base, left = c0 + w, base + w, left - w
        put(p, gslot).start()
        return carry

    lax.fori_loop(0, rows, row, 0)
    for p in (rows - 2, rows - 1):
        put(p, p % 2).wait()


def _last_kernel(g, cot, out, co_s, *bufs):
    n, na, cblk = g.shape
    occ = cot.shape[0]
    occ_p = co_s.shape[0]
    nt = len(bufs) // 2
    xs, ys = bufs[:nt], bufs[nt:]

    co_s[...] = jnp.zeros(co_s.shape, co_s.dtype)
    co_s[0:occ, :] = cot[...]
    for t in range(nt):
        w = min(LANES, cblk - t * LANES)
        xs[t][...] = g[:, :, t * LANES : t * LANES + w].astype(jnp.float32).reshape(n * na, w)
    for a in range(na):
        for t in range(nt):
            x = xs[t][pl.ds(a, n, stride=na), :].astype(jnp.bfloat16)
            y = jnp.dot(co_s[...], x, preferred_element_type=jnp.float32)
            ys[t][pl.ds(a, occ_p, stride=na), :] = y
    for t in range(nt):
        w = min(LANES, cblk - t * LANES)
        out[:, :, t * LANES : t * LANES + w] = ys[t][0 : occ * na, :].reshape(occ, na, w)


def solution(mesh):
    ndev = mesh.shape["dev"]

    def local_part(ao_rows, occ_coef, virt_coef):
        rows, n = ao_rows.shape[0], ao_rows.shape[1]
        occ, virt = occ_coef.shape[1], virt_coef.shape[1]
        occ_p = _up(occ, SUBL)
        cblk = occ * virt // ndev
        cot, cvt = occ_coef.T, virt_coef.T

        g = pl.pallas_call(
            functools.partial(_half_kernel, ndev, cblk),
            out_shape=jax.ShapeDtypeStruct((ndev, rows, virt, cblk), jnp.bfloat16),
            in_specs=[
                pl.BlockSpec(memory_space=pl.ANY),
                pl.BlockSpec(memory_space=pltpu.VMEM),
                pl.BlockSpec(memory_space=pltpu.VMEM),
            ],
            out_specs=pl.BlockSpec(memory_space=pl.ANY),
            scratch_shapes=[
                pltpu.VMEM((SLOTS, Q_CHUNK, n, n), jnp.bfloat16),
                pltpu.VMEM((occ_p, n), jnp.bfloat16),
                pltpu.VMEM((n, LANES), jnp.bfloat16),
                pltpu.VMEM((occ_p * HS, LANES), jnp.float32),
                pltpu.VMEM((2, ndev, virt, cblk), jnp.bfloat16),
                pltpu.SemaphoreType.DMA((SLOTS,)),
                pltpu.SemaphoreType.DMA((2,)),
            ],
            compiler_params=pltpu.CompilerParams(vmem_limit_bytes=48 * 2**20),
            name="first_three",
        )(ao_rows, cot, cvt)

        g = lax.all_to_all(g, "dev", 0, 0, tiled=True).reshape(ndev * rows, virt, cblk)

        a_blk = SUBL
        widths = [min(LANES, cblk - l) for l in range(0, cblk, LANES)]
        return pl.pallas_call(
            _last_kernel,
            grid=(virt // a_blk,),
            out_shape=jax.ShapeDtypeStruct((occ, virt, cblk), jnp.float32),
            in_specs=[
                pl.BlockSpec((n, a_blk, cblk), lambda k: (0, k, 0)),
                pl.BlockSpec((occ, n), lambda k: (0, 0)),
            ],
            out_specs=pl.BlockSpec((occ, a_blk, cblk), lambda k: (0, k, 0)),
            scratch_shapes=[pltpu.VMEM((occ_p, n), jnp.bfloat16)]
            + [pltpu.VMEM((n * a_blk, w), jnp.float32) for w in widths]
            + [pltpu.VMEM((occ_p * a_blk, w), jnp.float32) for w in widths],
            compiler_params=pltpu.CompilerParams(vmem_limit_bytes=32 * 2**20),
            name="last",
        )(g, cot)

    return jax.shard_map(
        local_part,
        mesh=mesh,
        in_specs=(P(("frag", "dev"), None, None, None), P("frag", None), P("frag", None)),
        out_specs=P("frag", None, "dev"),
        check_vma=False,
    )
```
